128 devices in a mesh: ia: 16 (over y, x), ja: 8 (over z, core).
Axes of the slice: x: 4, y: 4, z: 4, core: 2. Of those that a mesh axis runs over, the one named last changes fastest.
Arguments:
- slabs: bfloat16 [128, 512, 512], P(('ia', 'ja')), may hold values from -1.1953125 to 1.1953125
- pno_coef: bfloat16 [2048, 256, 128], P(('ia', 'ja')), may hold values from -0.375 to 0.375
- dom_blocks: int32 [2048, 2], P(('ia', 'ja')), may hold values from 0 to 3, as said below
- pair_first: int32 [2048], P(('ia', 'ja')), may hold values from 0 to 7
- pair_second: int32 [2048], P(('ia', 'ja')), may hold values from 0 to 15
- pno_energy: float32 [2048, 128], P(('ia', 'ja')), may hold values from 0.3 to 3
- pair_shift: float32 [2048], P(('ia', 'ja')), may hold values from 0.5 to 2
- margin_i: bfloat16 [2048, 16, 128, 128], P(('ia', 'ja')), may hold values from -0.5 to 0.5
- margin_j: bfloat16 [2048, 16, 128, 128], P(('ia', 'ja')), may hold values from -0.5 to 0.5
- couple_i: float32 [2048, 16], P(('ia', 'ja')), may hold values from -0.45 to 0.45
- couple_j: float32 [2048, 16], P(('ia', 'ja')), may hold values from -0.45 to 0.45
- ask_i: int32 [128, 16, 4], P(('ia', 'ja')), may hold values from 0 to 15, as said below
- ask_j: int32 [128, 8, 4], P(('ia', 'ja')), may hold values from 0 to 15, as said below
- link_i: int32 [2048, 16], P(('ia', 'ja')), may hold values from 0 to 63, as said below
- link_j: int32 [2048, 16], P(('ia', 'ja')), may hold values from 0 to 31, as said below
Outputs:
- amplitudes: float32 [2048, 128, 128], P(('ia', 'ja'))
- density: float32 [512, 512], P(('ia', 'ja'))
The draws below stay inside these ranges and needn't reach their ends.
Inputs may be any that keep to these rules, and one draw needn't show every extreme that they name: `dom_blocks`: the 2 blocks of a pair are distinct. `ask_i`: for each block g and each peer s, the 4 slots are distinct. `ask_j`: for each block g and each peer s, the 4 slots are distinct. `link_i`: within each aligned block of 16 pairs every value is named at least once. `link_j`: within each aligned block of 16 pairs every value is named at least once.
All inputs are finite; a program needn't handle non-finite values.
Results may differ from the reference program's by a relative error of at most 0.0045.
Values may be sent and summed in bfloat16 or wider, within the bound.
No kernel may reach another device: no remote copies, remote signals or barrier semaphores. Data moves between devices by JAX's collectives and lax.ppermute only.
A program may use at most 128 MiB of HBM per device.

```python
import math
import jax
import jax.numpy as jnp
from jax import lax

NPNO = 128
PAO = 512
AUX = 512
BLK = 128
DOMB = 2
NB_I = 16
NB_J = 16
ITERS = 2
PAIR_DEV = 16
NBLK = 4
DOM = 256
CAP_I = 4
CAP_J = 4
BLOCKS = 128
PAIRS = 2048
NOCC = 128
I_SPAN = 8
J_SPAN = 16
ROW_TABLE = 64
COL_TABLE = 32
N_IA = 16
N_JA = 8


def distinct_first(key, shape, pool_size, taken):
    scores = jax.random.randint(key, shape + (pool_size,), 0, 1 << 20) * pool_size + jnp.arange(pool_size, dtype=jnp.int32)
    ranking = jnp.argsort(scores, axis=-1, stable=True)
    return ranking[..., :taken].astype(jnp.int32)


def spread_links(key, table_size, per_block):

    def single(subkey):
        filler = jax.random.randint(subkey, (per_block - table_size,), 0, table_size).astype(jnp.int32)
        values = jnp.concatenate([jnp.arange(table_size, dtype=jnp.int32), filler])
        return jax.random.permutation(jax.random.fold_in(subkey, 7), values)
    return jax.vmap(single)(jax.random.split(key, BLOCKS))


def draw_dom_blocks(key, part):
    return distinct_first(jax.random.fold_in(key, 3), (PAIRS,), NBLK, DOMB)


def draw_ask_i(key, part):
    return distinct_first(jax.random.fold_in(key, 5), (BLOCKS, N_IA), PAIR_DEV, CAP_I)


def draw_ask_j(key, part):
    return distinct_first(jax.random.fold_in(key, 9), (BLOCKS, N_JA), PAIR_DEV, CAP_J)


def draw_link_i(key, part):
    return spread_links(jax.random.fold_in(key, 11), ROW_TABLE, PAIR_DEV * NB_I).reshape(PAIRS, NB_I)


def draw_link_j(key, part):
    return spread_links(jax.random.fold_in(key, 13), COL_TABLE, PAIR_DEV * NB_J).reshape(PAIRS, NB_J)


def set_ends(values, key, least, largest):
    longest = values.shape.index(max(values.shape))
    spots = []
    for shift in (0, 1):
        where = [jax.random.randint(jax.random.fold_in(key, axis), (), 0, length) for axis, length in enumerate(values.shape)]
        where[longest] = (where[longest] + shift) % values.shape[longest]
        spots.append(tuple(where))
    return values.at[spots[0]].set(least).at[spots[1]].set(largest)


def levels(rng, extent, cuts, least, high):
    factor_of = 1.0
    for axis_at, shards_of in cuts:
        heights = jax.random.uniform(jax.random.fold_in(jax.random.fold_in(rng, 6), axis_at), (shards_of,), jnp.float32, least / len(cuts), high / len(cuts))
        factor_of = factor_of * jnp.repeat(jnp.exp(heights), extent[axis_at] // shards_of).reshape((-1,) + (1,) * (len(extent) - 1 - axis_at))
    return factor_of


def gaussian(stream_key, dims, deviation, reach, shards=(), kind=jnp.bfloat16):
    values = jax.random.normal(stream_key, dims, jnp.float32) * deviation
    if len(shards) > 0:
        values = levels(stream_key, dims, shards, -0.22, 0.18) * values
    return jnp.clip(values, min=-reach, max=reach).astype(kind)


def setup_inputs(seed: int = 0) -> dict:
    streams_of = jax.random.split(jax.random.key(seed), 16)
    slabs = gaussian(streams_of[0], (NOCC, PAO, AUX), 0.2, 1.1953125, ((0, 128),))
    pno_coef = gaussian(streams_of[1], (PAIRS, DOM, NPNO), DOM ** -0.5, 0.375, ((0, 128),))
    dom_blocks = draw_dom_blocks(jax.random.fold_in(streams_of[15], 71), 0)
    pair_first = set_ends(jax.random.randint(streams_of[3], (PAIRS,), 0, I_SPAN), jax.random.fold_in(streams_of[3], 1), 0, I_SPAN - 1).astype(jnp.int32)
    pair_second = set_ends(jax.random.randint(streams_of[4], (PAIRS,), 0, J_SPAN), jax.random.fold_in(streams_of[4], 1), 0, J_SPAN - 1).astype(jnp.int32)
    pno_energy = jnp.clip(jnp.exp(math.log(3.0) - 2.3025851 * jax.random.uniform(streams_of[5], (PAIRS, NPNO), jnp.float32) ** levels(streams_of[5], (PAIRS, NPNO), ((0, 128),), -0.2, 0.2)), 0.3, 3.0)
    pair_shift = jnp.clip(jnp.exp(math.log(2.0) - 1.3862944 * jax.random.uniform(streams_of[6], (PAIRS,), jnp.float32) ** levels(streams_of[6], (PAIRS,), ((0, 128),), -0.2, 0.2)), 0.5, 2.0)
    margin_i = gaussian(streams_of[7], (PAIRS, NB_I, NPNO, NPNO), NPNO ** -0.5, 0.5, ((0, 128),))
    margin_j = gaussian(streams_of[8], (PAIRS, NB_J, NPNO, NPNO), NPNO ** -0.5, 0.5, ((0, 128),))
    couple_i = jnp.clip(jax.random.uniform(streams_of[9], (PAIRS, NB_I), jnp.float32, -0.45, 0.45) * levels(streams_of[9], (PAIRS, NB_I), ((0, 128),), -0.4, 0.0), -0.45, 0.45)
    couple_j = jnp.clip(jax.random.uniform(streams_of[10], (PAIRS, NB_J), jnp.float32, -0.45, 0.45) * levels(streams_of[10], (PAIRS, NB_J), ((0, 128),), -0.4, 0.0), -0.45, 0.45)
    ask_i = draw_ask_i(jax.random.fold_in(streams_of[15], 71), 0)
    ask_j = draw_ask_j(jax.random.fold_in(streams_of[15], 71), 0)
    link_i = draw_link_i(jax.random.fold_in(streams_of[15], 71), 0)
    link_j = draw_link_j(jax.random.fold_in(streams_of[15], 71), 0)
    return dict(slabs=slabs, pno_coef=pno_coef, dom_blocks=dom_blocks, pair_first=pair_first, pair_second=pair_second, pno_energy=pno_energy, pair_shift=pair_shift, margin_i=margin_i, margin_j=margin_j, couple_i=couple_i, couple_j=couple_j, ask_i=ask_i, ask_j=ask_j, link_i=link_i, link_j=link_j)


def coupled(near_blocks, margin_blocks, weights):
    left_side = jnp.einsum('nab,nbc->nac', margin_blocks.astype(jnp.float32), near_blocks.astype(jnp.float32)).astype(jnp.bfloat16)
    product = jnp.einsum('nac,ndc->nad', left_side.astype(jnp.float32), margin_blocks.astype(jnp.float32))
    return lax.optimization_barrier(jnp.sum(weights[:, None, None] * product, axis=0))

def reference(slabs, pno_coef, dom_blocks, pair_first, pair_second, pno_energy, pair_shift, margin_i, margin_j, couple_i, couple_j, ask_i, ask_j, link_i, link_j):
    pair_index = jnp.arange(PAIRS, dtype=jnp.int32)
    owner_block = pair_index // PAIR_DEV
    block_row = owner_block // N_JA
    block_col = owner_block % N_JA
    first_orbital = block_row * N_JA + pair_first
    second_orbital = pair_second * N_JA + block_col
    slab_blocks = slabs.reshape(NOCC * NBLK, BLK, AUX)

    def pair_exchange(packed):
        orbital_one, orbital_two, coefs, domains = packed
        rows_one = slab_blocks[orbital_one * NBLK + domains].reshape(DOM, AUX)
        rows_two = slab_blocks[orbital_two * NBLK + domains].reshape(DOM, AUX)
        projected_one = jnp.dot(coefs.T, rows_one, preferred_element_type=jnp.float32).astype(jnp.bfloat16)
        projected_two = jnp.dot(coefs.T, rows_two, preferred_element_type=jnp.float32).astype(jnp.bfloat16)
        return jnp.dot(projected_one, projected_two.T, preferred_element_type=jnp.float32)
    exchange_ints = lax.map(pair_exchange, (first_orbital, second_orbital, pno_coef, dom_blocks))
    denominator = pno_energy[:, :, None] + pno_energy[:, None, :] + pair_shift[:, None, None]
    amplitudes = -exchange_ints / denominator
    peer_first = link_i // CAP_I
    slot_first = link_i % CAP_I
    near_first = (peer_first * N_JA + block_col[:, None]) * PAIR_DEV + ask_i[owner_block[:, None], peer_first, slot_first]
    peer_second = link_j // CAP_J
    slot_second = link_j % CAP_J
    near_second = (block_row[:, None] * N_JA + peer_second) * PAIR_DEV + ask_j[owner_block[:, None], peer_second, slot_second]
    for iteration in range(ITERS):
        sent = amplitudes.astype(jnp.bfloat16)

        def pair_coupling(packed):
            index_one, margin_one, weight_one, index_two, margin_two, weight_two = packed
            return coupled(sent[index_one], margin_one, weight_one) + coupled(sent[index_two], margin_two, weight_two)
        coupling = lax.map(pair_coupling, (near_first, margin_i, couple_i, near_second, margin_j, couple_j))
        residual = exchange_ints + denominator * amplitudes + coupling
        amplitudes = amplitudes - residual / denominator
    sent = amplitudes.astype(jnp.bfloat16)

    def accumulate(running, packed):
        amp_block, coefs, domains = packed
        square = (jnp.dot(amp_block, amp_block.T, preferred_element_type=jnp.float32) + jnp.dot(amp_block.T, amp_block, preferred_element_type=jnp.float32)).astype(jnp.bfloat16)
        mapped = jnp.dot(coefs, square, preferred_element_type=jnp.float32).astype(jnp.bfloat16)
        domain_density = jnp.dot(mapped, coefs.T, preferred_element_type=jnp.float32)
        select = (domains[:, None] == jnp.arange(NBLK, dtype=jnp.int32)[None, :]).astype(jnp.float32)
        placed = jnp.einsum('kg,lh,krlc->grhc', select, select, domain_density.reshape(DOMB, BLK, DOMB, BLK), precision=lax.Precision.HIGHEST)
        return (running + placed.reshape(PAO, PAO), None)
    running, unused = lax.scan(accumulate, jnp.zeros((PAO, PAO), jnp.float32), (sent, pno_coef, dom_blocks))
    density = running * (1.0 / math.sqrt(PAIRS))
    return (amplitudes, density)
```

```python
import functools
import math

import jax
import jax.numpy as jnp
from jax import lax
from jax.experimental import pallas as pl
from jax.experimental.pallas import tpu as pltpu
from jax.sharding import Mesh
from jax.sharding import PartitionSpec as P

BLK = 128
ITERS = 2
IA = ("y", "x")
JA = ("z", "c")
ALL = ("y", "x", "z", "c")
F32 = jnp.float32
BF16 = jnp.bfloat16
GROUP = 4
VMEM_LIMIT = 62 * 1024 * 1024


SMEM = pl.BlockSpec(memory_space=pltpu.SMEM)
WHOLE = pl.BlockSpec(memory_space=pltpu.VMEM)
FAR = pl.BlockSpec(memory_space=pltpu.HBM)


def shifted(value, axis, step):
    return lax.ppermute(value, axis, [(i, (i + step) % 4) for i in range(4)])


def to_peer(value, far, near):
    moves = [
        (z * 2 + c, ((z + far) % 4) * 2 + (c + near) % 2) for z in range(4) for c in range(2)
    ]
    return lax.ppermute(value, JA, moves)


def dot(a, b):
    return jnp.dot(a, b, preferred_element_type=F32)


def dot_t(a, b):
    return lax.dot_general(a, b, (((1,), (1,)), ((), ())), preferred_element_type=F32)


def around(value, axis, mid):
    f = shifted(value, axis, 1)
    b = shifted(value, axis, -1)
    return [value, f, b, shifted(f[:mid], axis, 1), shifted(b[mid:], axis, -1)]


def with_asks(rows, ask):
    tile = jnp.zeros((16, rows.shape[1]), BF16)
    tile = lax.dynamic_update_slice(tile, ask.astype(BF16), (0, 0))
    return jnp.concatenate([rows, tile], axis=0)


def ring_place(delta):
    return jnp.where(delta == 0, 0, jnp.where(delta == 3, 1, delta + 1))


PLACE_DELTA = (0, 3, 1, 2)


def in_groups(count, one):
    def group(g, carry):
        one([g * GROUP + i for i in range(GROUP)])
        return carry

    lax.fori_loop(0, count // GROUP, group, 0)


def fetch(pieces, code, row, target, sem):
    row = pl.multiple_of(row, 16)
    for j, ref in enumerate(pieces):

        @pl.when(code == j)
        def _(ref=ref):
            pltpu.make_async_copy(ref.at[pl.ds(row, BLK)], target, sem).start()


def arrived(rows, sems, p):
    for k in range(2):
        target = rows.at[p, pl.ds(k * BLK, BLK)]
        pltpu.make_async_copy(target, target, sems.at[p, k]).wait()


def named(tiles, own, owner_of, out):
    pick = lax.broadcasted_iota(jnp.int32, (16, BLK), 0) == own
    for j in range(tiles.shape[0]):
        row = jnp.sum(jnp.where(pick, tiles[j].astype(F32), 0.0), axis=0, keepdims=True)
        out[pl.ds(owner_of(j), 1)] = row.astype(jnp.int32)


def first_kernel(where, first, dom, coef_t, *refs):
    pieces, (out, asked), (rows, sems, tiles, tile_sem) = refs[:10], refs[10:12], refs[12:]
    z, c = where[2], where[3]

    def start(p, carry):
        orb = first[p]
        place = ring_place((orb // 2 - z) & 3)
        base = ((orb % 2 - c) & 1) * 5
        for k in range(2):
            block = dom[p, k]
            low = block >= 2
            code = jnp.where(place == 3, jnp.where(low, 4, 3), place)
            row = jnp.where((place == 3) & low, block - 2, block) * BLK
            fetch(pieces, base + code, row, rows.at[p, pl.ds(k * BLK, BLK)], sems.at[p, k])
        return carry

    copies = []
    for j in range(8):
        side, place = j // 4, j % 4
        ref, row = (pieces[side * 5 + 4], 256) if place == 3 else (pieces[side * 5 + place], 512)
        copies.append(
            pltpu.make_async_copy(ref.at[pl.ds(row, 16), pl.ds(0, BLK)], tiles.at[j], tile_sem.at[j])
        )
        copies[-1].start()
    lax.fori_loop(0, out.shape[0], start, 0)
    for copy in copies:
        copy.wait()

    def owner_of(j):
        return ((z + PLACE_DELTA[j % 4]) & 3) * 2 + ((c + j // 4) & 1)

    named(tiles, z * 2 + c, owner_of, asked)

    def one(group):
        for p in group:
            arrived(rows, sems, p)
        for p in group:
            out[p] = dot(coef_t[p], rows[p]).astype(BF16)

    in_groups(out.shape[0], one)


def pack(sent, where, asked_i, asked_j, send_i, send_j):
    def rows(peer, carry):
        for r in range(4):
            send_i[peer * 4 + r] = sent[asked_i[peer, r]]
        return carry

    lax.fori_loop(0, 16, rows, 0)
    for d, ref in enumerate(send_j):
        peer = ((where[2] + d // 2) & 3) * 2 + ((where[3] + d % 2) & 1)
        for r in range(4):
            ref[r] = sent[asked_j[peer, r]]


def exchange_kernel(where, second, dom, asked_j, coef_t, projected, scale, *refs):
    pieces, (exch, asked, send_i), send_j = refs[:10], refs[10:13], refs[13:21]
    rows, sems, tiles, tile_sem, sent, asked_i, asked_sem = refs[21:]
    y, x = where[0], where[1]
    units = (2 * BLK + 16, 2 * BLK)

    def start(p, carry):
        orb = second[p]
        place_y = ring_place((orb // 4 - y) & 3)
        place_x = ring_place((orb % 4 - x) & 3)
        for k in range(2):
            block = dom[p, k]
            colour = block // 2
            outer = jnp.where(colour == 0, place_y, place_x)
            inner = jnp.where(colour == 0, place_x, place_y)
            late = (outer == 3) & (inner >= 2)
            code = colour * 5 + outer + jnp.where(late, 1, 0)
            row = (inner - jnp.where(late, 2, 0)) * jnp.where(colour == 0, units[0], units[1])
            row = row + block % 2 * BLK
            fetch(pieces, code, row, rows.at[p, pl.ds(k * BLK, BLK)], sems.at[p, k])
        return carry

    lax.fori_loop(0, exch.shape[0], start, 0)
    copies = []
    for j in range(16):
        outer, inner = j // 4, j % 4
        late = outer == 3 and inner >= 2
        row = (inner - 2 * late) * units[0] + 2 * BLK
        copies.append(
            pltpu.make_async_copy(
                pieces[outer + late].at[pl.ds(row, 16), pl.ds(0, BLK)],
                tiles.at[j],
                tile_sem.at[j],
            )
        )
        copies[-1].start()

    def one(group):
        for p in group:
            arrived(rows, sems, p)
        other = [dot(coef_t[p], rows[p]).astype(BF16) for p in group]
        for p, right in zip(group, other):
            value = dot_t(projected[p], right)
            exch[p] = value
            sent[p] = (value * scale[p]).astype(BF16)

    in_groups(exch.shape[0], one)
    for copy in copies:
        copy.wait()

    def owner_of(j):
        return ((y + PLACE_DELTA[j // 4]) & 3) * 4 + ((x + PLACE_DELTA[j % 4]) & 3)

    named(tiles, y * 4 + x, owner_of, asked)
    to_scalars = pltpu.make_async_copy(asked, asked_i, asked_sem)
    to_scalars.start()
    to_scalars.wait()
    pack(sent, where, asked_i, asked_j, send_i, send_j)


def coupling(p, margin, table, entry, couple, i):
    lane = lax.broadcasted_iota(jnp.int32, (1, 2 * BLK), 1)
    zero = jnp.zeros((BLK, BLK), BF16)
    total = jnp.zeros((BLK, BLK), F32)
    for n in range(0, 16, 2):
        both = jnp.concatenate([margin[i, n], margin[i, n + 1]], axis=1)
        near = jnp.concatenate(
            [
                jnp.concatenate([table[entry(p, n)], zero], axis=1),
                jnp.concatenate([zero, table[entry(p, n + 1)]], axis=1),
            ],
            axis=0,
        )
        weight = jnp.where(lane < BLK, couple[p, n], couple[p, n + 1])
        left = (dot(both, near) * weight).astype(BF16)
        total = total + dot_t(left, both)
    return total


def group_of(count):
    first = pl.program_id(0) * count
    return [(first + i, i) for i in range(count)]


def second_kind_kernel(where, link, couple, margin, *refs):
    parts, out, table = refs[:8], refs[8], refs[9]

    @pl.when(pl.program_id(0) == 0)
    def _():
        for d, ref in enumerate(parts):
            table[pl.ds(d * 4, 4)] = ref[...]

    def entry(p, n):
        value = link[p, n]
        s = value // 4
        d = ((s // 2 - where[2]) & 3) * 2 + ((s % 2 - where[3]) & 1)
        return d * 4 + value % 4

    for p, i in group_of(out.shape[0]):
        out[i] = coupling(p, margin, table, entry, couple, i)


def middle_kernel(where, link, couple, asked_i, asked_j, margin, table, other, exch, scale, *refs):
    send_i, send_j, sent = refs[0], refs[1:9], refs[9]
    for p, i in group_of(exch.shape[0]):
        total = coupling(p, margin, table, lambda p, n: link[p, n], couple, i)
        sent[p] = ((exch[i] + (other[i] + total)) * scale[i]).astype(BF16)

    @pl.when(pl.program_id(0) == pl.num_programs(0) - 1)
    def _():
        pack(sent, where, asked_i, asked_j, send_i, send_j)


def last_kernel(factor, link, couple, dom, margin, table, other, exch, scale, coef, *refs):
    amp, dens, acc = refs

    @pl.when(pl.program_id(0) == 0)
    def _():
        acc[...] = jnp.zeros_like(acc)

    group = range(exch.shape[0])
    values = []
    for p, i in group_of(exch.shape[0]):
        total = coupling(p, margin, table, lambda p, n: link[p, n], couple, i)
        values.append((exch[i] + (other[i] + total)) * scale[i])
        amp[i] = values[i]
    sent = [value.astype(BF16) for value in values]
    square = [(dot_t(v, v) + dot(v.T, v)).astype(BF16) for v in sent]
    mapped = [dot(coef[i], square[i]).astype(BF16) for i in group]
    blocks = [dot_t(mapped[i], coef[i]) for i in group]
    for (p, i), block in zip(group_of(exch.shape[0]), blocks):
        for k in range(2):
            for m in range(2):
                at = dom[p, k], dom[p, m]
                acc[at] = acc[at] + block[k * BLK : (k + 1) * BLK, m * BLK : (m + 1) * BLK]

    @pl.when(pl.program_id(0) == pl.num_programs(0) - 1)
    def _():
        for k in range(4):
            for m in range(4):
                dens[k * BLK : (k + 1) * BLK, m * BLK : (m + 1) * BLK] = (
                    acc[k, m] * factor
                ).astype(BF16)


def params():
    return pltpu.CompilerParams(vmem_limit_bytes=VMEM_LIMIT)


def cost(flops, size):
    return pl.CostEstimate(flops=flops, bytes_accessed=size, transcendentals=0)


def per_pair(shape):
    return pl.BlockSpec((GROUP, *shape), lambda p: (p,) + (0,) * len(shape))


def fixed(shape):
    return pl.BlockSpec(shape, lambda p: (0,) * len(shape))


def body(
    slabs,
    pno_coef,
    dom_blocks,
    pair_first,
    pair_second,
    pno_energy,
    pair_shift,
    margin_i,
    margin_j,
    couple_i,
    couple_j,
    ask_i,
    ask_j,
    link_i,
    link_j,
):
    pairs, domain, pno = pno_coef.shape
    pao, aux = slabs.shape[1:]
    where = jnp.stack([lax.axis_index(a) for a in ALL]).astype(jnp.int32)
    slab = slabs.reshape(pao, aux)
    top = with_asks(slab[: pao // 2], ask_i.reshape(ask_i.shape[1:]))
    by_x = jnp.concatenate(around(top, "x", BLK), axis=0)
    by_y = jnp.concatenate(around(slab[pao // 2 :], "y", BLK), axis=0)
    pieces = around(by_x, "y", by_x.shape[0] // 2) + around(by_y, "x", by_y.shape[0] // 2)
    line = around(with_asks(slab, ask_j.reshape(ask_j.shape[1:])), "z", pao // 2)
    line += [lax.ppermute(v, "c", [(0, 1), (1, 0)]) for v in line]
    scale = -1.0 / (pno_energy[:, :, None] + pno_energy[:, None, :] + pair_shift[:, None, None])
    coef_t = pno_coef.swapaxes(1, 2)

    block = jax.ShapeDtypeStruct((pairs, pno, pno), F32)
    send_types = [jax.ShapeDtypeStruct((64, pno, pno), BF16)] + [
        jax.ShapeDtypeStruct((4, pno, pno), BF16)
    ] * 8
    fetched = [pltpu.VMEM((pairs, domain, aux), BF16), pltpu.SemaphoreType.DMA((pairs, 2))]
    projected, asked_j = pl.pallas_call(
        first_kernel,
        out_shape=[
            jax.ShapeDtypeStruct((pairs, pno, aux), BF16),
            jax.ShapeDtypeStruct((8, BLK), jnp.int32),
        ],
        in_specs=[SMEM] * 3 + [WHOLE] + [FAR] * 10,
        out_specs=[WHOLE] * 2,
        scratch_shapes=fetched
        + [pltpu.VMEM((8, 16, BLK), BF16), pltpu.SemaphoreType.DMA((8,))],
        compiler_params=params(),
        cost_estimate=cost(pairs * pno * domain * aux * 2, 6 << 20),
        name="project_first",
    )(where, pair_first, dom_blocks, coef_t, *line)

    exch, asked_i, *sends = pl.pallas_call(
        exchange_kernel,
        out_shape=[block, jax.ShapeDtypeStruct((16, BLK), jnp.int32)] + send_types,
        in_specs=[SMEM] * 4 + [WHOLE] * 3 + [FAR] * 10,
        out_specs=[WHOLE] * 11,
        scratch_shapes=fetched
        + [
            pltpu.VMEM((16, 16, BLK), BF16),
            pltpu.SemaphoreType.DMA((16,)),
            pltpu.VMEM((pairs, pno, pno), BF16),
            pltpu.SMEM((16, BLK), jnp.int32),
            pltpu.SemaphoreType.DMA,
        ],
        compiler_params=params(),
        cost_estimate=cost(pairs * pno * domain * aux * 3, 10 << 20),
        name="exchange",
    )(where, pair_second, dom_blocks, asked_j, coef_t, projected, scale, *pieces)

    work = 16 * pairs * pno**3 * 4
    table_spec = fixed((64, pno, pno))
    margin_spec = per_pair((16, pno, pno))
    block_spec = per_pair((pno, pno))
    for iteration in range(ITERS):
        send_i, send_j = sends[0], sends[1:]
        table_i = lax.all_to_all(
            send_i.reshape(16, 4, pno, pno), IA, split_axis=0, concat_axis=0, tiled=True
        ).reshape(64, pno, pno)
        parts = [send_j[0]]
        for d in range(1, 8):
            back = ((-(d // 2)) % 4) * 2 + d % 2
            parts.append(to_peer(send_j[back], back // 2, back % 2))
        other = pl.pallas_call(
            second_kind_kernel,
            grid=(pairs // GROUP,),
            out_shape=block,
            in_specs=[SMEM] * 3 + [margin_spec] + [fixed((4, pno, pno))] * 8,
            out_specs=block_spec,
            scratch_shapes=[pltpu.VMEM((32, pno, pno), BF16)],
            compiler_params=params(),
            cost_estimate=cost(work, 10 << 20),
            name="couple_second",
        )(where, link_j, couple_j, margin_j, *parts)
        if iteration < ITERS - 1:
            sends = pl.pallas_call(
                middle_kernel,
                grid=(pairs // GROUP,),
                out_shape=send_types,
                in_specs=[SMEM] * 5 + [margin_spec, table_spec] + [block_spec] * 3,
                out_specs=[table_spec] + [fixed((4, pno, pno))] * 8,
                scratch_shapes=[pltpu.VMEM((pairs, pno, pno), BF16)],
                compiler_params=params(),
                cost_estimate=cost(work, 12 << 20),
                name="couple_first",
            )(where, link_i, couple_i, asked_i, asked_j, margin_i, table_i, other, exch, scale)
        else:
            factor = 1.0 / math.sqrt(pairs * lax.axis_size(ALL))
            amplitudes, partial_sum = pl.pallas_call(
                functools.partial(last_kernel, factor),
                grid=(pairs // GROUP,),
                out_shape=[block, jax.ShapeDtypeStruct((pao, pao), BF16)],
                in_specs=[SMEM] * 3
                + [margin_spec, table_spec]
                + [block_spec] * 3
                + [per_pair((domain, pno))],
                out_specs=[block_spec, fixed((pao, pao))],
                scratch_shapes=[pltpu.VMEM((4, 4, BLK, BLK), F32)],
                compiler_params=params(),
                cost_estimate=cost(work, 14 << 20),
                name="couple_last",
            )(link_i, couple_i, dom_blocks, margin_i, table_i, other, exch, scale, pno_coef)
    split = partial_sum.reshape(-1, 4, pao)
    got = lax.all_to_all(split, ALL, split_axis=0, concat_axis=0, tiled=True)
    return amplitudes, jnp.sum(got.astype(F32), axis=0)


def solution(mesh):
    split = Mesh(mesh.devices.reshape(4, 4, 4, 2), ALL)
    ranks = (3, 3, 2, 1, 1, 2, 1, 4, 4, 2, 2, 3, 3, 2, 2)
    placed = tuple(P(ALL, *(None,) * (rank - 1)) for rank in ranks)
    return jax.shard_map(
        body,
        mesh=split,
        in_specs=placed,
        out_specs=(P(ALL, None, None), P(ALL, None)),
        check_vma=False,
    )
```

```python
import functools
import math

import jax
import jax.numpy as jnp
from jax import lax
from jax.experimental import pallas as pl
from jax.experimental.pallas import tpu as pltpu
from jax.sharding import Mesh
from jax.sharding import PartitionSpec as P

BLK = 128
ITERS = 2
IA = ("y", "x")
JA = ("z", "c")
ALL = ("y", "x", "z", "c")
F32 = jnp.float32
BF16 = jnp.bfloat16
GROUP = 4
VMEM_LIMIT = 62 * 1024 * 1024


SMEM = pl.BlockSpec(memory_space=pltpu.SMEM)
WHOLE = pl.BlockSpec(memory_space=pltpu.VMEM)
FAR = pl.BlockSpec(memory_space=pltpu.HBM)


def shifted(value, axis, step):
    return lax.ppermute(value, axis, [(i, (i + step) % 4) for i in range(4)])


def to_peer(value, far, near):
    moves = [
        (z * 2 + c, ((z + far) % 4) * 2 + (c + near) % 2) for z in range(4) for c in range(2)
    ]
    return lax.ppermute(value, JA, moves)


def dot(a, b):
    return jnp.dot(a, b, preferred_element_type=F32)


def dot_t(a, b):
    return lax.dot_general(a, b, (((1,), (1,)), ((), ())), preferred_element_type=F32)


def neighbours(value, axis):
    return [shifted(value, axis, 1), shifted(value, axis, -1), shifted(value, axis, 2)]


def ring_of_halves(low, high, axis):
    f_low = shifted(low, axis, 1)
    b_high = shifted(high, axis, -1)
    f_high = shifted(high, axis, 1)
    b_low = shifted(low, axis, -1)
    return [low, high, f_low, f_high, b_low, b_high], f_low, b_high


def with_asks(rows, ask):
    tile = jnp.zeros((16, rows.shape[1]), BF16)
    tile = lax.dynamic_update_slice(tile, ask.astype(BF16), (0, 0))
    return jnp.concatenate([rows, tile], axis=0)


def ring_place(delta):
    return jnp.where(delta == 0, 0, jnp.where(delta == 3, 1, delta + 1))


PLACE_DELTA = (0, 3, 1, 2)


def in_groups(count, one):
    def group(g, carry):
        one([g * GROUP + i for i in range(GROUP)])
        return carry

    lax.fori_loop(0, count // GROUP, group, 0)


def fetch(pieces, code, row, target, sem):
    row = pl.multiple_of(row, 16)
    for j, ref in enumerate(pieces):

        @pl.when(code == j)
        def _(ref=ref):
            pltpu.make_async_copy(ref.at[pl.ds(row, BLK)], target, sem).start()


def arrived(rows, sems, p):
    for k in range(2):
        target = rows.at[p, pl.ds(k * BLK, BLK)]
        pltpu.make_async_copy(target, target, sems.at[p, k]).wait()


def named(tiles, own, owner_of, out):
    pick = lax.broadcasted_iota(jnp.int32, (16, BLK), 0) == own
    for j in range(tiles.shape[0]):
        row = jnp.sum(jnp.where(pick, tiles[j].astype(F32), 0.0), axis=0, keepdims=True)
        out[pl.ds(owner_of(j), 1)] = row.astype(jnp.int32)


def first_kernel(where, first, dom, coef_t, *refs):
    pieces, (out, asked), (rows, sems, tiles, tile_sem) = refs[:8], refs[8:10], refs[10:]
    z, c = where[2], where[3]

    def start(p, carry):
        orb = first[p]
        code = ((orb % 2 - c) & 1) * 4 + ring_place((orb // 2 - z) & 3)
        for k in range(2):
            target = rows.at[p, pl.ds(k * BLK, BLK)]
            fetch(pieces, code, dom[p, k] * BLK, target, sems.at[p, k])
        return carry

    copies = []
    for j in range(8):
        copies.append(
            pltpu.make_async_copy(
                pieces[j].at[pl.ds(4 * BLK, 16), pl.ds(0, BLK)], tiles.at[j], tile_sem.at[j]
            )
        )
        copies[-1].start()
    lax.fori_loop(0, out.shape[0], start, 0)
    for copy in copies:
        copy.wait()

    def owner_of(j):
        return ((z + PLACE_DELTA[j % 4]) & 3) * 2 + ((c + j // 4) & 1)

    named(tiles, z * 2 + c, owner_of, asked)

    def one(group):
        for p in group:
            arrived(rows, sems, p)
        for p in group:
            out[p] = dot(coef_t[p], rows[p]).astype(BF16)

    in_groups(out.shape[0], one)


def pack(sent, where, asked_i, asked_j, send_i, send_j):
    def rows(peer, carry):
        for r in range(4):
            send_i[peer * 4 + r] = sent[asked_i[peer, r]]
        return carry

    lax.fori_loop(0, 16, rows, 0)
    for d, ref in enumerate(send_j):
        peer = ((where[2] + d // 2) & 3) * 2 + ((where[3] + d % 2) & 1)
        for r in range(4):
            ref[r] = sent[asked_j[peer, r]]


def exchange_kernel(where, second, dom, asked_j, coef_t, projected, scale, *refs):
    pieces, (exch, asked, send_i), send_j = refs[:16], refs[16:19], refs[19:27]
    rows, sems, tiles, tile_sem, sent, asked_i, asked_sem = refs[27:]
    y, x = where[0], where[1]
    units = (2 * BLK + 16, 2 * BLK)

    def start(p, carry):
        orb = second[p]
        place_y = ring_place((orb // 4 - y) & 3)
        place_x = ring_place((orb % 4 - x) & 3)
        for k in range(2):
            block = dom[p, k]
            colour = block // 2
            outer = jnp.where(colour == 0, place_y, place_x)
            inner = jnp.where(colour == 0, place_x, place_y)
            code = colour * 8 + outer * 2 + inner // 2
            row = inner % 2 * jnp.where(colour == 0, units[0], units[1])
            row = row + block % 2 * BLK
            fetch(pieces, code, row, rows.at[p, pl.ds(k * BLK, BLK)], sems.at[p, k])
        return carry

    copies = []
    for j in range(16):
        row = j % 2 * units[0] + 2 * BLK
        copies.append(
            pltpu.make_async_copy(
                pieces[j // 2].at[pl.ds(row, 16), pl.ds(0, BLK)], tiles.at[j], tile_sem.at[j]
            )
        )
        copies[-1].start()
    lax.fori_loop(0, exch.shape[0], start, 0)
    for copy in copies:
        copy.wait()

    def owner_of(j):
        return ((y + PLACE_DELTA[j // 4]) & 3) * 4 + ((x + PLACE_DELTA[j % 4]) & 3)

    named(tiles, y * 4 + x, owner_of, asked)
    to_scalars = pltpu.make_async_copy(asked, asked_i, asked_sem)
    to_scalars.start()

    def one(group):
        for p in group:
            arrived(rows, sems, p)
        other = [dot(coef_t[p], rows[p]).astype(BF16) for p in group]
        for p, right in zip(group, other):
            value = dot_t(projected[p], right)
            exch[p] = value
            sent[p] = (value * scale[p]).astype(BF16)

    in_groups(exch.shape[0], one)
    to_scalars.wait()
    pack(sent, where, asked_i, asked_j, send_i, send_j)


def lefts(p, margin, table, entry, couple):
    lane = lax.broadcasted_iota(jnp.int32, (1, 2 * BLK), 1)
    zero = jnp.zeros((BLK, BLK), BF16)
    result = []
    for n in range(0, 16, 2):
        both = jnp.concatenate([margin[p, n], margin[p, n + 1]], axis=1)
        near = jnp.concatenate(
            [
                jnp.concatenate([table[entry(p, n)], zero], axis=1),
                jnp.concatenate([zero, table[entry(p, n + 1)]], axis=1),
            ],
            axis=0,
        )
        weight = jnp.where(lane < BLK, couple[p, n], couple[p, n + 1])
        result.append((dot(both, near) * weight).astype(BF16))
    return result


def rights(p, margin, left):
    total = jnp.zeros((BLK, BLK), F32)
    for n in range(0, 16, 2):
        both = jnp.concatenate([margin[p, n], margin[p, n + 1]], axis=1)
        total = total + dot_t(left[n // 2], both)
    return total


def couplings(group, margin, table, entry, couple):
    totals, last = [], None
    for p in group:
        left = lefts(p, margin, table, entry, couple)
        if last is not None:
            totals.append(rights(*last))
        last = p, margin, left
    return totals + [rights(*last)]


class Loads:
    def __init__(self, sources, targets, sem):
        self.sources, self.targets, self.sem = sources, targets, sem
        self.margin_i, self.margin_j, self.table_i, self.table_j, self.exch, self.scale = targets
        self.groups = self.exch.shape[0] // GROUP
        for copy in self.parts():
            copy.start()
        for g in range(self.groups):
            self.second(g).start()
            if g == 0:
                self.table().start()
            for copy in self.first(g):
                copy.start()

    def grouped(self, source, target, g, kind):
        at = pl.ds(g * GROUP, GROUP)
        sem = self.sem.at[9 + kind * self.groups + g]
        return pltpu.make_async_copy(source.at[at], target.at[at], sem)

    def parts(self):
        return [
            pltpu.make_async_copy(ref, self.table_j.at[pl.ds(d * 4, 4)], self.sem.at[d])
            for d, ref in enumerate(self.sources[5])
        ]

    def table(self):
        return pltpu.make_async_copy(self.sources[2], self.table_i, self.sem.at[8])

    def second(self, g):
        return self.grouped(self.sources[1], self.margin_j, g, 0)

    def first(self, g):
        return [
            self.grouped(self.sources[0], self.margin_i, g, 1),
            self.grouped(self.sources[3], self.exch, g, 2),
            self.grouped(self.sources[4], self.scale, g, 3),
        ]


def update(loads, g, where, link_i, couple_i, link_j, couple_j):
    def entry_i(p, n):
        return link_i[p, n]

    def entry_j(p, n):
        value = link_j[p, n]
        s = value // 4
        d = ((s // 2 - where[2]) & 3) * 2 + ((s % 2 - where[3]) & 1)
        return d * 4 + value % 4

    group = [g * GROUP + i for i in range(GROUP)]
    loads.second(g).wait()
    parts_j = couplings(group, loads.margin_j, loads.table_j, entry_j, couple_j)

    @pl.when(g == 0)
    def _():
        loads.table().wait()

    for copy in loads.first(g):
        copy.wait()
    parts_i = couplings(group, loads.margin_i, loads.table_i, entry_i, couple_i)
    return [
        (p, (loads.exch[p] + (i + j)) * loads.scale[p]) for p, i, j in zip(group, parts_i, parts_j)
    ]


def middle_kernel(where, link_i, couple_i, link_j, couple_j, asked_i, asked_j, *refs):
    sources, send_i, send_j, sent = (*refs[:5], refs[5:13]), refs[13], refs[14:22], refs[22]
    loads = Loads(sources, refs[23:29], refs[29])
    for copy in loads.parts():
        copy.wait()

    def group(g, carry):
        for p, value in update(loads, g, where, link_i, couple_i, link_j, couple_j):
            sent[p] = value.astype(BF16)
        return carry

    lax.fori_loop(0, loads.groups, group, 0)
    pack(sent, where, asked_i, asked_j, send_i, send_j)


def last_kernel(factor, where, link_i, couple_i, link_j, couple_j, dom, coef, *refs):
    sources, amp, dens, acc = (*refs[:5], refs[5:13]), refs[13], refs[14], refs[15]
    loads = Loads(sources, refs[16:22], refs[22])
    acc[...] = jnp.zeros_like(acc)
    for copy in loads.parts():
        copy.wait()

    def group(g, carry):
        sent = []
        for p, value in update(loads, g, where, link_i, couple_i, link_j, couple_j):
            amp[p] = value
            sent.append((p, value.astype(BF16)))
        square = [(p, (dot_t(v, v) + dot(v.T, v)).astype(BF16)) for p, v in sent]
        mapped = [(p, dot(coef[p], v).astype(BF16)) for p, v in square]
        blocks = [(p, dot_t(v, coef[p])) for p, v in mapped]
        for p, block in blocks:
            for k in range(2):
                for m in range(2):
                    at = dom[p, k], dom[p, m]
                    acc[at] = acc[at] + block[k * BLK : (k + 1) * BLK, m * BLK : (m + 1) * BLK]
        return carry

    lax.fori_loop(0, loads.groups, group, 0)
    for k in range(4):
        for m in range(4):
            dens[k * BLK : (k + 1) * BLK, m * BLK : (m + 1) * BLK] = (acc[k, m] * factor).astype(
                BF16
            )


def params():
    return pltpu.CompilerParams(vmem_limit_bytes=VMEM_LIMIT)


def cost(flops, size):
    return pl.CostEstimate(flops=flops, bytes_accessed=size, transcendentals=0)


def body(
    slabs,
    pno_coef,
    dom_blocks,
    pair_first,
    pair_second,
    pno_energy,
    pair_shift,
    margin_i,
    margin_j,
    couple_i,
    couple_j,
    ask_i,
    ask_j,
    link_i,
    link_j,
):
    pairs, domain, pno = pno_coef.shape
    pao, aux = slabs.shape[1:]
    where = jnp.stack([lax.axis_index(a) for a in ALL]).astype(jnp.int32)
    slab = slabs.reshape(pao, aux)
    top = with_asks(slab[: pao // 2], ask_i.reshape(ask_i.shape[1:]))
    bottom = slab[pao // 2 :]
    line = with_asks(slab, ask_j.reshape(ask_j.shape[1:]))
    near_x = neighbours(top, "x")
    near_y = neighbours(bottom, "y")
    lines = [line] + neighbours(line, "z")
    by_x, relay_x, back_x = ring_of_halves(
        jnp.concatenate([top, near_x[0]], axis=0), jnp.concatenate(near_x[1:], axis=0), "y"
    )
    by_y, relay_y, back_y = ring_of_halves(
        jnp.concatenate([bottom, near_y[0]], axis=0), jnp.concatenate(near_y[1:], axis=0), "x"
    )
    lines += [lax.ppermute(v, "c", [(0, 1), (1, 0)]) for v in lines]
    by_x += [shifted(relay_x, "y", 1), shifted(back_x, "y", -1)]
    by_y += [shifted(relay_y, "x", 1), shifted(back_y, "x", -1)]
    pieces = by_x + by_y
    scale = -1.0 / (pno_energy[:, :, None] + pno_energy[:, None, :] + pair_shift[:, None, None])
    coef_t = pno_coef.swapaxes(1, 2)

    block = jax.ShapeDtypeStruct((pairs, pno, pno), F32)
    send_types = [jax.ShapeDtypeStruct((64, pno, pno), BF16)] + [
        jax.ShapeDtypeStruct((4, pno, pno), BF16)
    ] * 8
    fetched = [pltpu.VMEM((pairs, domain, aux), BF16), pltpu.SemaphoreType.DMA((pairs, 2))]
    projected, asked_j = pl.pallas_call(
        first_kernel,
        out_shape=[
            jax.ShapeDtypeStruct((pairs, pno, aux), BF16),
            jax.ShapeDtypeStruct((8, BLK), jnp.int32),
        ],
        in_specs=[SMEM] * 3 + [WHOLE] + [FAR] * 8,
        out_specs=[WHOLE] * 2,
        scratch_shapes=fetched
        + [pltpu.VMEM((8, 16, BLK), BF16), pltpu.SemaphoreType.DMA((8,))],
        compiler_params=params(),
        cost_estimate=cost(pairs * pno * domain * aux * 2, 6 << 20),
        name="project_first",
    )(where, pair_first, dom_blocks, coef_t, *lines)

    exch, asked_i, *sends = pl.pallas_call(
        exchange_kernel,
        out_shape=[block, jax.ShapeDtypeStruct((16, BLK), jnp.int32)] + send_types,
        in_specs=[SMEM] * 4 + [WHOLE] * 3 + [FAR] * 16,
        out_specs=[WHOLE] * 11,
        scratch_shapes=fetched
        + [
            pltpu.VMEM((16, 16, BLK), BF16),
            pltpu.SemaphoreType.DMA((16,)),
            pltpu.VMEM((pairs, pno, pno), BF16),
            pltpu.SMEM((16, BLK), jnp.int32),
            pltpu.SemaphoreType.DMA,
        ],
        compiler_params=params(),
        cost_estimate=cost(pairs * pno * domain * aux * 3, 10 << 20),
        name="exchange",
    )(where, pair_second, dom_blocks, asked_j, coef_t, projected, scale, *pieces)

    work = 32 * pairs * pno**3 * 4
    margin = (pairs, 16, pno, pno)
    scratch = [
        pltpu.VMEM(margin, BF16),
        pltpu.VMEM(margin, BF16),
        pltpu.VMEM((64, pno, pno), BF16),
        pltpu.VMEM((32, pno, pno), BF16),
        pltpu.VMEM((pairs, pno, pno), F32),
        pltpu.VMEM((pairs, pno, pno), F32),
        pltpu.SemaphoreType.DMA((9 + 4 * pairs // GROUP,)),
    ]
    for iteration in range(ITERS):
        send_i, send_j = sends[0], sends[1:]
        table_i = lax.all_to_all(
            send_i.reshape(16, 4, pno, pno), IA, split_axis=0, concat_axis=0, tiled=True
        ).reshape(64, pno, pno)
        parts = {0: send_j[0]}
        for d in (6, 2, 7, 3, 4, 5, 1):
            back = ((-(d // 2)) % 4) * 2 + d % 2
            parts[d] = to_peer(send_j[back], back // 2, back % 2)
        known = (where, link_i, couple_i, link_j, couple_j)
        large = (margin_i, margin_j, table_i, exch, scale, *(parts[d] for d in range(8)))
        if iteration < ITERS - 1:
            sends = pl.pallas_call(
                middle_kernel,
                out_shape=send_types,
                in_specs=[SMEM] * 7 + [FAR] * 13,
                out_specs=[WHOLE] * 9,
                scratch_shapes=[pltpu.VMEM((pairs, pno, pno), BF16)] + scratch,
                compiler_params=params(),
                cost_estimate=cost(work, 24 << 20),
                name="iteration",
            )(*known, asked_i, asked_j, *large)
        else:
            factor = 1.0 / math.sqrt(pairs * lax.axis_size(ALL))
            amplitudes, partial_sum = pl.pallas_call(
                functools.partial(last_kernel, factor),
                out_shape=[block, jax.ShapeDtypeStruct((pao, pao), BF16)],
                in_specs=[SMEM] * 6 + [WHOLE] + [FAR] * 13,
                out_specs=[WHOLE] * 2,
                scratch_shapes=[pltpu.VMEM((4, 4, BLK, BLK), F32)] + scratch,
                compiler_params=params(),
                cost_estimate=cost(work, 26 << 20),
                name="last_iteration",
            )(*known, dom_blocks, pno_coef, *large)
    split = partial_sum.reshape(-1, 4, pao)
    got = lax.all_to_all(split, ALL, split_axis=0, concat_axis=0, tiled=True)
    return amplitudes, jnp.sum(got.astype(F32), axis=0)


def solution(mesh):
    split = Mesh(mesh.devices.reshape(4, 4, 4, 2), ALL)
    ranks = (3, 3, 2, 1, 1, 2, 1, 4, 4, 2, 2, 3, 3, 2, 2)
    placed = tuple(P(ALL, *(None,) * (rank - 1)) for rank in ranks)
    return jax.shard_map(
        body,
        mesh=split,
        in_specs=placed,
        out_specs=(P(ALL, None, None), P(ALL, None)),
        check_vma=False,
    )
```

```python
import functools
import math

import jax
import jax.numpy as jnp
from jax import lax
from jax.experimental import pallas as pl
from jax.experimental.pallas import tpu as pltpu
from jax.sharding import Mesh
from jax.sharding import PartitionSpec as P


BLK = 128
ITERS = 2
IA = ("y", "x")
JA = ("z", "c")
ALL = ("y", "x", "z", "c")
F32 = jnp.float32
BF16 = jnp.bfloat16
GROUP = 4
GROUPS = 4
VMEM_LIMIT = 62 * 1024 * 1024


SMEM = pl.BlockSpec(memory_space=pltpu.SMEM)
WHOLE = pl.BlockSpec(memory_space=pltpu.VMEM)
FAR = pl.BlockSpec(memory_space=pltpu.HBM)


def shifted(value, axis, step):
    return lax.ppermute(value, axis, [(i, (i + step) % 4) for i in range(4)])


def to_peer(value, far, near):
    moves = [
        (z * 2 + c, ((z + far) % 4) * 2 + (c + near) % 2) for z in range(4) for c in range(2)
    ]
    return lax.ppermute(value, JA, moves)


def dot(a, b):
    return jnp.dot(a, b, preferred_element_type=F32)


def dot_t(a, b):
    return lax.dot_general(a, b, (((1,), (1,)), ((), ())), preferred_element_type=F32)


def neighbours(value, axis):
    got = []
    for step in (1, -1, 2):
        got.append(shifted(value, axis, step))
    return got


def ring_of_halves(low, high, axis):
    f_low = shifted(low, axis, 1)
    b_low = shifted(low, axis, -1)
    b_high = shifted(high, axis, -1)
    f_high = shifted(high, axis, 1)
    return [low, high, f_low, f_high, b_low, b_high], f_low, b_high


def across(lines):
    got = []
    for value in lines:
        got.append(lax.ppermute(value, "c", [(0, 1), (1, 0)]))
    return got


def with_asks(rows, ask):
    tile = jnp.zeros((16, rows.shape[1]), BF16)
    tile = lax.dynamic_update_slice(tile, ask.astype(BF16), (0, 0))
    return jnp.concatenate([rows, tile], axis=0)


def ring_place(delta):
    return jnp.where(delta == 0, 0, jnp.where(delta == 3, 1, delta + 1))


PLACE_DELTA = (0, 3, 1, 2)


def in_groups(count, one):
    def group(g, carry):
        one([g * GROUP + i for i in range(GROUP)])
        return carry

    lax.fori_loop(0, count // GROUP, group, 0)


def fetch(pieces, code, row, target, sem):
    row = pl.multiple_of(row, 16)
    for j, ref in enumerate(pieces):

        @pl.when(code == j)
        def _(ref=ref):
            pltpu.make_async_copy(ref.at[pl.ds(row, BLK)], target, sem).start()


def arrived(rows, sems, p):
    for k in range(2):
        target = rows.at[p, pl.ds(k * BLK, BLK)]
        pltpu.make_async_copy(target, target, sems.at[p, k]).wait()


def named(tiles, own, owner_of, out):
    pick = lax.broadcasted_iota(jnp.int32, (16, BLK), 0) == own
    for j in range(tiles.shape[0]):
        row = jnp.sum(jnp.where(pick, tiles[j].astype(F32), 0.0), axis=0, keepdims=True)
        out[pl.ds(owner_of(j), 1)] = row.astype(jnp.int32)


def first_kernel(where, first, dom, coef_t, *refs):
    pieces, (out, asked), (rows, sems, tiles, tile_sem) = refs[:8], refs[8:10], refs[10:]
    z, c = where[2], where[3]

    def start(p, carry):
        orb = first[p]
        code = ((orb % 2 - c) & 1) * 4 + ring_place((orb // 2 - z) & 3)
        for k in range(2):
            target = rows.at[p, pl.ds(k * BLK, BLK)]
            fetch(pieces, code, dom[p, k] * BLK, target, sems.at[p, k])
        return carry

    copies = []
    for j in range(8):
        copies.append(
            pltpu.make_async_copy(
                pieces[j].at[pl.ds(4 * BLK, 16), pl.ds(0, BLK)], tiles.at[j], tile_sem.at[j]
            )
        )
        copies[-1].start()
    lax.fori_loop(0, out.shape[0], start, 0)
    for copy in copies:
        copy.wait()

    def owner_of(j):
        return ((z + PLACE_DELTA[j % 4]) & 3) * 2 + ((c + j // 4) & 1)

    named(tiles, z * 2 + c, owner_of, asked)

    def one(group):
        for p in group:
            arrived(rows, sems, p)
        for p in group:
            out[p] = dot(coef_t[p], rows[p]).astype(BF16)

    in_groups(out.shape[0], one)


def pack(sent, where, asked_i, asked_j, send_i, send_j):
    def rows(peer, carry):
        for r in range(4):
            send_i[peer * 4 + r] = sent[asked_i[peer, r]]
        return carry

    lax.fori_loop(0, 16, rows, 0)
    for d, ref in enumerate(send_j):
        peer = ((where[2] + d // 2) & 3) * 2 + ((where[3] + d % 2) & 1)
        for r in range(4):
            ref[r] = sent[asked_j[peer, r]]


def exchange_kernel(where, second, dom, asked_j, coef_t, projected, scale, *refs):
    pieces, (exch, asked, send_i), send_j = refs[:16], refs[16:19], refs[19:27]
    rows, sems, tiles, tile_sem, sent, asked_i, asked_sem = refs[27:]
    y, x = where[0], where[1]
    units = (2 * BLK + 16, 2 * BLK)

    def start(p, carry):
        orb = second[p]
        place_y = ring_place((orb // 4 - y) & 3)
        place_x = ring_place((orb % 4 - x) & 3)
        for k in range(2):
            block = dom[p, k]
            colour = block // 2
            outer = jnp.where(colour == 0, place_y, place_x)
            inner = jnp.where(colour == 0, place_x, place_y)
            code = colour * 8 + outer * 2 + inner // 2
            row = inner % 2 * jnp.where(colour == 0, units[0], units[1])
            row = row + block % 2 * BLK
            fetch(pieces, code, row, rows.at[p, pl.ds(k * BLK, BLK)], sems.at[p, k])
        return carry

    copies = []
    for j in range(16):
        row = j % 2 * units[0] + 2 * BLK
        copies.append(
            pltpu.make_async_copy(
                pieces[j // 2].at[pl.ds(row, 16), pl.ds(0, BLK)], tiles.at[j], tile_sem.at[j]
            )
        )
        copies[-1].start()
    lax.fori_loop(0, exch.shape[0], start, 0)
    for copy in copies:
        copy.wait()

    def owner_of(j):
        return ((y + PLACE_DELTA[j // 4]) & 3) * 4 + ((x + PLACE_DELTA[j % 4]) & 3)

    named(tiles, y * 4 + x, owner_of, asked)
    to_scalars = pltpu.make_async_copy(asked, asked_i, asked_sem)
    to_scalars.start()

    def one(group):
        for p in group:
            arrived(rows, sems, p)
        other = [dot(coef_t[p], rows[p]).astype(BF16) for p in group]
        for p, right in zip(group, other):
            value = dot_t(projected[p], right)
            exch[p] = value
            sent[p] = (value * scale[p]).astype(BF16)

    in_groups(exch.shape[0], one)
    to_scalars.wait()
    pack(sent, where, asked_i, asked_j, send_i, send_j)


def lefts(p, margin, table, entry, couple):
    lane = lax.broadcasted_iota(jnp.int32, (1, 2 * BLK), 1)
    zero = jnp.zeros((BLK, BLK), BF16)
    result = []
    for n in range(0, 16, 2):
        both = jnp.concatenate([margin[p, n], margin[p, n + 1]], axis=1)
        near = jnp.concatenate(
            [
                jnp.concatenate([table[entry(p, n)], zero], axis=1),
                jnp.concatenate([zero, table[entry(p, n + 1)]], axis=1),
            ],
            axis=0,
        )
        weight = jnp.where(lane < BLK, couple[p, n], couple[p, n + 1])
        result.append((dot(both, near) * weight).astype(BF16))
    return result


def rights(p, margin, left):
    total = jnp.zeros((BLK, BLK), F32)
    for n in range(0, 16, 2):
        both = jnp.concatenate([margin[p, n], margin[p, n + 1]], axis=1)
        total = total + dot_t(left[n // 2], both)
    return total


def couplings(group, margin, table, entry, couple):
    totals, last = [], None
    for p in group:
        left = lefts(p, margin, table, entry, couple)
        if last is not None:
            totals.append(rights(*last))
        last = p, margin, left
    return totals + [rights(*last)]


class Loads:
    def __init__(self, tables, arrays, sem):
        self.tables, self.arrays, self.sem = tables, arrays, sem
        for copy in self.whole():
            copy.start()
        for g in range(GROUPS):
            for copy in self.group(g):
                copy.start()

    def whole(self):
        return [
            pltpu.make_async_copy(source, target, self.sem.at[i])
            for i, (source, target) in enumerate(self.tables)
        ]

    def group(self, g):
        at = pl.ds(g * GROUP, GROUP)
        base = len(self.tables)
        return [
            pltpu.make_async_copy(
                source.at[at], target.at[at], self.sem.at[base + i * GROUPS + g]
            )
            for i, (source, target) in enumerate(self.arrays)
        ]

    def each_group(self, step):
        for copy in self.whole():
            copy.wait()

        def group(g, carry):
            for copy in self.group(g):
                copy.wait()
            step([g * GROUP + i for i in range(GROUP)])
            return carry

        lax.fori_loop(0, GROUPS, group, 0)


def second_kind_kernel(where, link, couple, margin_far, exch_far, *refs):
    parts, out, margin, exch, table, sem = refs[:8], *refs[8:]
    tables = [(ref, table.at[pl.ds(d * 4, 4)]) for d, ref in enumerate(parts)]
    loads = Loads(tables, [(margin_far, margin), (exch_far, exch)], sem)

    def entry(p, n):
        value = link[p, n]
        s = value // 4
        d = ((s // 2 - where[2]) & 3) * 2 + ((s % 2 - where[3]) & 1)
        return d * 4 + value % 4

    def step(group):
        for p, total in zip(group, couplings(group, margin, table, entry, couple)):
            out[p] = exch[p] + total

    loads.each_group(step)


def first_kind(loaded, link, couple):
    margin_far, table_far, base_far, scale_far, margin, table, base, scale, sem = loaded
    arrays = [(margin_far, margin), (base_far, base), (scale_far, scale)]
    loads = Loads([(table_far, table)], arrays, sem)

    def values(group):
        totals = couplings(group, margin, table, lambda p, n: link[p, n], couple)
        return [(p, (base[p] + total) * scale[p]) for p, total in zip(group, totals)]

    return loads, values


def middle_kernel(where, link, couple, asked_i, asked_j, *refs):
    far, send_i, send_j, sent = refs[:4], refs[4], refs[5:13], refs[13]
    loads, values = first_kind(far + refs[14:], link, couple)

    def step(group):
        for p, value in values(group):
            sent[p] = value.astype(BF16)

    loads.each_group(step)
    pack(sent, where, asked_i, asked_j, send_i, send_j)


def last_kernel(factor, link, couple, dom, coef, *refs):
    far, (amp, dens, acc) = refs[:4], refs[4:7]
    loads, values = first_kind(far + refs[7:], link, couple)
    acc[...] = jnp.zeros_like(acc)

    def step(group):
        sent = []
        for p, value in values(group):
            amp[p] = value
            sent.append((p, value.astype(BF16)))
        square = [(p, (dot_t(v, v) + dot(v.T, v)).astype(BF16)) for p, v in sent]
        mapped = [(p, dot(coef[p], v).astype(BF16)) for p, v in square]
        blocks = [(p, dot_t(v, coef[p])) for p, v in mapped]
        for p, block in blocks:
            for k in range(2):
                for m in range(2):
                    at = dom[p, k], dom[p, m]
                    acc[at] = acc[at] + block[k * BLK : (k + 1) * BLK, m * BLK : (m + 1) * BLK]

    loads.each_group(step)
    for k in range(4):
        for m in range(4):
            dens[k * BLK : (k + 1) * BLK, m * BLK : (m + 1) * BLK] = (acc[k, m] * factor).astype(
                BF16
            )


def params():
    return pltpu.CompilerParams(vmem_limit_bytes=VMEM_LIMIT)


def cost(flops, size):
    return pl.CostEstimate(flops=flops, bytes_accessed=size, transcendentals=0)


def steps(
    slabs,
    pno_coef,
    dom_blocks,
    pair_first,
    pair_second,
    pno_energy,
    pair_shift,
    margin_i,
    margin_j,
    couple_i,
    couple_j,
    ask_i,
    ask_j,
    link_i,
    link_j,
):
    pairs, domain, pno = pno_coef.shape
    pao, aux = slabs.shape[1:]
    where = jnp.stack([lax.axis_index(a) for a in ALL]).astype(jnp.int32)
    slab = slabs.reshape(pao, aux)
    top = with_asks(slab[: pao // 2], ask_i.reshape(ask_i.shape[1:]))
    bottom = slab[pao // 2 :]
    line = with_asks(slab, ask_j.reshape(ask_j.shape[1:]))
    near_x = neighbours(top, "x")
    near_y = neighbours(bottom, "y")
    lines = [line] + neighbours(line, "z")
    by_x, relay_x, back_x = ring_of_halves(
        jnp.concatenate([top, near_x[0]], axis=0), jnp.concatenate(near_x[1:], axis=0), "y"
    )
    by_y, relay_y, back_y = ring_of_halves(
        jnp.concatenate([bottom, near_y[0]], axis=0), jnp.concatenate(near_y[1:], axis=0), "x"
    )
    lines += across(lines)
    by_x += [shifted(relay_x, "y", 1), shifted(back_x, "y", -1)]
    by_y += [shifted(relay_y, "x", 1), shifted(back_y, "x", -1)]
    pieces = by_x + by_y
    scale = -1.0 / (pno_energy[:, :, None] + pno_energy[:, None, :] + pair_shift[:, None, None])
    coef_t = pno_coef.swapaxes(1, 2)

    block = jax.ShapeDtypeStruct((pairs, pno, pno), F32)
    send_types = [jax.ShapeDtypeStruct((64, pno, pno), BF16)] + [
        jax.ShapeDtypeStruct((4, pno, pno), BF16)
    ] * 8
    fetched = [pltpu.VMEM((pairs, domain, aux), BF16), pltpu.SemaphoreType.DMA((pairs, 2))]
    projected, asked_j = pl.pallas_call(
        first_kernel,
        out_shape=[
            jax.ShapeDtypeStruct((pairs, pno, aux), BF16),
            jax.ShapeDtypeStruct((8, BLK), jnp.int32),
        ],
        in_specs=[SMEM] * 3 + [WHOLE] + [FAR] * 8,
        out_specs=[WHOLE] * 2,
        scratch_shapes=fetched
        + [pltpu.VMEM((8, 16, BLK), BF16), pltpu.SemaphoreType.DMA((8,))],
        compiler_params=params(),
        cost_estimate=cost(pairs * pno * domain * aux * 2, 6 << 20),
        name="project_first",
    )(where, pair_first, dom_blocks, coef_t, *lines)

    exch, asked_i, *sends = pl.pallas_call(
        exchange_kernel,
        out_shape=[block, jax.ShapeDtypeStruct((16, BLK), jnp.int32)] + send_types,
        in_specs=[SMEM] * 4 + [WHOLE] * 3 + [FAR] * 16,
        out_specs=[WHOLE] * 11,
        scratch_shapes=fetched
        + [
            pltpu.VMEM((16, 16, BLK), BF16),
            pltpu.SemaphoreType.DMA((16,)),
            pltpu.VMEM((pairs, pno, pno), BF16),
            pltpu.SMEM((16, BLK), jnp.int32),
            pltpu.SemaphoreType.DMA,
        ],
        compiler_params=params(),
        cost_estimate=cost(pairs * pno * domain * aux * 3, 10 << 20),
        name="exchange",
    )(where, pair_second, dom_blocks, asked_j, coef_t, projected, scale, *pieces)

    work = 16 * pairs * pno**3 * 4
    margin = pltpu.VMEM((pairs, 16, pno, pno), BF16)
    values = pltpu.VMEM((pairs, pno, pno), F32)
    first_scratch = [
        margin,
        pltpu.VMEM((64, pno, pno), BF16),
        values,
        values,
        pltpu.SemaphoreType.DMA((1 + 3 * GROUPS,)),
    ]
    for iteration in range(ITERS):
        send_i, send_j = sends[0], sends[1:]
        table_i = lax.all_to_all(
            send_i.reshape(16, 4, pno, pno), IA, split_axis=0, concat_axis=0, tiled=True
        ).reshape(64, pno, pno)
        parts = {0: send_j[0]}
        for d in (6, 2, 7, 3, 4, 5, 1):
            back = ((-(d // 2)) % 4) * 2 + d % 2
            parts[d] = to_peer(send_j[back], back // 2, back % 2)
        base = pl.pallas_call(
            second_kind_kernel,
            out_shape=block,
            in_specs=[SMEM] * 3 + [FAR] * 10,
            out_specs=WHOLE,
            scratch_shapes=[
                margin,
                values,
                pltpu.VMEM((32, pno, pno), BF16),
                pltpu.SemaphoreType.DMA((8 + 2 * GROUPS,)),
            ],
            compiler_params=params(),
            cost_estimate=cost(work, 12 << 20),
            name="couple_second",
        )(where, link_j, couple_j, margin_j, exch, *(parts[d] for d in range(8)))
        large = (margin_i, table_i, base, scale)
        if iteration < ITERS - 1:
            sends = pl.pallas_call(
                middle_kernel,
                out_shape=send_types,
                in_specs=[SMEM] * 5 + [FAR] * 4,
                out_specs=[WHOLE] * 9,
                scratch_shapes=[pltpu.VMEM((pairs, pno, pno), BF16)] + first_scratch,
                compiler_params=params(),
                cost_estimate=cost(work, 14 << 20),
                name="couple_first",
            )(where, link_i, couple_i, asked_i, asked_j, *large)
        else:
            factor = 1.0 / math.sqrt(pairs * lax.axis_size(ALL))
            amplitudes, partial_sum = pl.pallas_call(
                functools.partial(last_kernel, factor),
                out_shape=[block, jax.ShapeDtypeStruct((pao, pao), BF16)],
                in_specs=[SMEM] * 3 + [WHOLE] + [FAR] * 4,
                out_specs=[WHOLE] * 2,
                scratch_shapes=[pltpu.VMEM((4, 4, BLK, BLK), F32)] + first_scratch,
                compiler_params=params(),
                cost_estimate=cost(work, 16 << 20),
                name="couple_last",
            )(link_i, couple_i, dom_blocks, pno_coef, *large)
    split = partial_sum.reshape(-1, 4, pao)
    got = lax.all_to_all(split, ALL, split_axis=0, concat_axis=0, tiled=True)
    return amplitudes, jnp.sum(got.astype(F32), axis=0)


def solution(mesh):
    split = Mesh(mesh.devices.reshape(4, 4, 4, 2), ALL)
    ranks = (3, 3, 2, 1, 1, 2, 1, 4, 4, 2, 2, 3, 3, 2, 2)
    placed = tuple(P(ALL, *(None,) * (rank - 1)) for rank in ranks)
    return jax.shard_map(
        steps,
        mesh=split,
        in_specs=placed,
        out_specs=(P(ALL, None, None), P(ALL, None)),
        check_vma=False,
    )
```

```python
import functools
import math

import jax
import jax.numpy as jnp
from jax import lax
from jax.experimental import pallas as pl
from jax.experimental.pallas import tpu as pltpu
from jax.sharding import Mesh
from jax.sharding import PartitionSpec as P


BLK = 128
ITERS = 2
IA = ("y", "x")
JA = ("z", "c")
ALL = ("y", "x", "z", "c")
F32 = jnp.float32
BF16 = jnp.bfloat16
GROUP = 4
GROUPS = 4
VMEM_LIMIT = 62 * 1024 * 1024


SMEM = pl.BlockSpec(memory_space=pltpu.SMEM)
WHOLE = pl.BlockSpec(memory_space=pltpu.VMEM)
FAR = pl.BlockSpec(memory_space=pltpu.HBM)


def shifted(value, axis, step):
    return lax.ppermute(value, axis, [(i, (i + step) % 4) for i in range(4)])


def to_peer(value, far, near):
    moves = [
        (z * 2 + c, ((z + far) % 4) * 2 + (c + near) % 2) for z in range(4) for c in range(2)
    ]
    return lax.ppermute(value, JA, moves)


def dot(a, b):
    return jnp.dot(a, b, preferred_element_type=F32)


def dot_t(a, b):
    return lax.dot_general(a, b, (((1,), (1,)), ((), ())), preferred_element_type=F32)


def neighbours(value, axis):
    got = []
    for step in (1, -1, 2):
        got.append(shifted(value, axis, step))
    return got


def ring_of_halves(low, high, axis):
    f_low = shifted(low, axis, 1)
    b_low = shifted(low, axis, -1)
    b_high = shifted(high, axis, -1)
    f_high = shifted(high, axis, 1)
    return [low, high, f_low, f_high, b_low, b_high], f_low, b_high


def across(lines):
    got = []
    for value in lines:
        got.append(lax.ppermute(value, "c", [(0, 1), (1, 0)]))
    return got


def with_asks(rows, ask):
    tile = jnp.zeros((16, rows.shape[1]), BF16)
    tile = lax.dynamic_update_slice(tile, ask.astype(BF16), (0, 0))
    return jnp.concatenate([rows, tile], axis=0)


def ring_place(delta):
    return jnp.where(delta == 0, 0, jnp.where(delta == 3, 1, delta + 1))


PLACE_DELTA = (0, 3, 1, 2)


def in_groups(count, one):
    def group(g, carry):
        one([g * GROUP + i for i in range(GROUP)])
        return carry

    lax.fori_loop(0, count // GROUP, group, 0)


def fetch(pieces, code, row, target, sem):
    row = pl.multiple_of(row, 16)
    for j, ref in enumerate(pieces):

        @pl.when(code == j)
        def _(ref=ref):
            pltpu.make_async_copy(ref.at[pl.ds(row, BLK)], target, sem).start()


def arrived(rows, sems, p):
    for k in range(2):
        target = rows.at[p, pl.ds(k * BLK, BLK)]
        pltpu.make_async_copy(target, target, sems.at[p, k]).wait()


def named(tiles, own, owner_of, out):
    pick = lax.broadcasted_iota(jnp.int32, (16, BLK), 0) == own
    for j in range(tiles.shape[0]):
        row = jnp.sum(jnp.where(pick, tiles[j].astype(F32), 0.0), axis=0, keepdims=True)
        out[pl.ds(owner_of(j), 1)] = row.astype(jnp.int32)


def first_kernel(where, first, dom, coef_t, *refs):
    pieces, (out, asked), (rows, sems, tiles, tile_sem) = refs[:8], refs[8:10], refs[10:]
    z, c = where[2], where[3]

    def start(p, carry):
        orb = first[p]
        code = ((orb % 2 - c) & 1) * 4 + ring_place((orb // 2 - z) & 3)
        for k in range(2):
            target = rows.at[p, pl.ds(k * BLK, BLK)]
            fetch(pieces, code, dom[p, k] * BLK, target, sems.at[p, k])
        return carry

    copies = []
    for j in range(8):
        copies.append(
            pltpu.make_async_copy(
                pieces[j].at[pl.ds(4 * BLK, 16), pl.ds(0, BLK)], tiles.at[j], tile_sem.at[j]
            )
        )
        copies[-1].start()
    lax.fori_loop(0, out.shape[0], start, 0)
    for copy in copies:
        copy.wait()

    def owner_of(j):
        return ((z + PLACE_DELTA[j % 4]) & 3) * 2 + ((c + j // 4) & 1)

    named(tiles, z * 2 + c, owner_of, asked)

    def one(group):
        for p in group:
            arrived(rows, sems, p)
        for p in group:
            out[p] = dot(coef_t[p], rows[p]).astype(BF16)

    in_groups(out.shape[0], one)


def pack(sent, where, asked_i, asked_j, send_i, send_j):
    def rows(peer, carry):
        for r in range(4):
            send_i[peer * 4 + r] = sent[asked_i[peer, r]]
        return carry

    lax.fori_loop(0, 16, rows, 0)
    for d, ref in enumerate(send_j):
        peer = ((where[2] + d // 2) & 3) * 2 + ((where[3] + d % 2) & 1)
        for r in range(4):
            ref[r] = sent[asked_j[peer, r]]


def exchange_kernel(where, second, dom, asked_j, coef_far, projected_far, scale_far, *refs):
    pieces, (exch, asked, send_i), send_j = refs[:16], refs[16:19], refs[19:27]
    rows, sems, tiles, tile_sem, sent, asked_i, asked_sem = refs[27:34]
    coef_t, projected, scale, load_sem = refs[34:]
    y, x = where[0], where[1]
    units = (2 * BLK + 16, 2 * BLK)

    def start(p, carry):
        orb = second[p]
        place_y = ring_place((orb // 4 - y) & 3)
        place_x = ring_place((orb % 4 - x) & 3)
        for k in range(2):
            block = dom[p, k]
            colour = block // 2
            outer = jnp.where(colour == 0, place_y, place_x)
            inner = jnp.where(colour == 0, place_x, place_y)
            code = colour * 8 + outer * 2 + inner // 2
            row = inner % 2 * jnp.where(colour == 0, units[0], units[1])
            row = row + block % 2 * BLK
            fetch(pieces, code, row, rows.at[p, pl.ds(k * BLK, BLK)], sems.at[p, k])
        return carry

    copies = []
    for j in range(16):
        row = j % 2 * units[0] + 2 * BLK
        copies.append(
            pltpu.make_async_copy(
                pieces[j // 2].at[pl.ds(row, 16), pl.ds(0, BLK)], tiles.at[j], tile_sem.at[j]
            )
        )
        copies[-1].start()
    lax.fori_loop(0, exch.shape[0], start, 0)
    arrays = [(coef_far, coef_t), (projected_far, projected), (scale_far, scale)]
    loads = Loads([], arrays, load_sem)
    for copy in copies:
        copy.wait()

    def owner_of(j):
        return ((y + PLACE_DELTA[j // 4]) & 3) * 4 + ((x + PLACE_DELTA[j % 4]) & 3)

    named(tiles, y * 4 + x, owner_of, asked)
    to_scalars = pltpu.make_async_copy(asked, asked_i, asked_sem)
    to_scalars.start()

    def one(group):
        for p in group:
            arrived(rows, sems, p)
        other = [dot(coef_t[p], rows[p]).astype(BF16) for p in group]
        for p, right in zip(group, other):
            value = dot_t(projected[p], right)
            exch[p] = value
            sent[p] = (value * scale[p]).astype(BF16)

    loads.each_group(one)
    to_scalars.wait()
    pack(sent, where, asked_i, asked_j, send_i, send_j)


def lefts(p, margin, table, entry, couple):
    lane = lax.broadcasted_iota(jnp.int32, (1, 2 * BLK), 1)
    zero = jnp.zeros((BLK, BLK), BF16)
    result = []
    for n in range(0, 16, 2):
        both = jnp.concatenate([margin[p, n], margin[p, n + 1]], axis=1)
        near = jnp.concatenate(
            [
                jnp.concatenate([table[entry(p, n)], zero], axis=1),
                jnp.concatenate([zero, table[entry(p, n + 1)]], axis=1),
            ],
            axis=0,
        )
        weight = jnp.where(lane < BLK, couple[p, n], couple[p, n + 1])
        result.append((dot(both, near) * weight).astype(BF16))
    return result


def rights(p, margin, left):
    total = jnp.zeros((BLK, BLK), F32)
    for n in range(0, 16, 2):
        both = jnp.concatenate([margin[p, n], margin[p, n + 1]], axis=1)
        total = total + dot_t(left[n // 2], both)
    return total


def couplings(group, margin, table, entry, couple):
    totals, last = [], None
    for p in group:
        left = lefts(p, margin, table, entry, couple)
        if last is not None:
            totals.append(rights(*last))
        last = p, margin, left
    return totals + [rights(*last)]


class Loads:
    def __init__(self, tables, arrays, sem):
        self.tables, self.arrays, self.sem = tables, arrays, sem
        for copy in self.whole():
            copy.start()
        for g in range(GROUPS):
            for copy in self.group(g):
                copy.start()

    def whole(self):
        return [
            pltpu.make_async_copy(source, target, self.sem.at[i])
            for i, (source, target) in enumerate(self.tables)
        ]

    def group(self, g):
        at = pl.ds(g * GROUP, GROUP)
        base = len(self.tables)
        return [
            pltpu.make_async_copy(
                source.at[at], target.at[at], self.sem.at[base + i * GROUPS + g]
            )
            for i, (source, target) in enumerate(self.arrays)
        ]

    def each_group(self, step):
        for copy in self.whole():
            copy.wait()

        def group(g, carry):
            for copy in self.group(g):
                copy.wait()
            step([g * GROUP + i for i in range(GROUP)])
            return carry

        lax.fori_loop(0, GROUPS, group, 0)


def second_kind_kernel(where, link, couple, margin_far, exch_far, *refs):
    parts, out, margin, exch, table, sem = refs[:8], *refs[8:]
    tables = [(ref, table.at[pl.ds(d * 4, 4)]) for d, ref in enumerate(parts)]
    loads = Loads(tables, [(margin_far, margin), (exch_far, exch)], sem)

    def entry(p, n):
        value = link[p, n]
        s = value // 4
        d = ((s // 2 - where[2]) & 3) * 2 + ((s % 2 - where[3]) & 1)
        return d * 4 + value % 4

    def step(group):
        for p, total in zip(group, couplings(group, margin, table, entry, couple)):
            out[p] = exch[p] + total

    loads.each_group(step)


def first_kind(loaded, link, couple, extra=()):
    margin_far, table_far, base_far, scale_far, margin, table, base, scale, sem = loaded
    arrays = [(margin_far, margin), (base_far, base), (scale_far, scale)]
    loads = Loads([(table_far, table)], arrays + list(extra), sem)

    def values(group):
        totals = couplings(group, margin, table, lambda p, n: link[p, n], couple)
        return [(p, (base[p] + total) * scale[p]) for p, total in zip(group, totals)]

    return loads, values


def middle_kernel(where, link, couple, asked_i, asked_j, *refs):
    far, send_i, send_j, sent = refs[:4], refs[4], refs[5:13], refs[13]
    loads, values = first_kind(far + refs[14:], link, couple)

    def step(group):
        for p, value in values(group):
            sent[p] = value.astype(BF16)

    loads.each_group(step)
    pack(sent, where, asked_i, asked_j, send_i, send_j)


def last_kernel(factor, link, couple, dom, coef_far, *refs):
    far, (amp, dens, acc) = refs[:4], refs[4:7]
    coef = refs[12]
    loads, values = first_kind(far + refs[7:12], link, couple, [(coef_far, coef)])
    acc[...] = jnp.zeros_like(acc)

    def step(group):
        sent = []
        for p, value in values(group):
            amp[p] = value
            sent.append((p, value.astype(BF16)))
        square = [(p, (dot_t(v, v) + dot(v.T, v)).astype(BF16)) for p, v in sent]
        mapped = [(p, dot(coef[p], v).astype(BF16)) for p, v in square]
        blocks = [(p, dot_t(v, coef[p])) for p, v in mapped]
        for p, block in blocks:
            for k in range(2):
                for m in range(2):
                    at = dom[p, k], dom[p, m]
                    acc[at] = acc[at] + block[k * BLK : (k + 1) * BLK, m * BLK : (m + 1) * BLK]

    loads.each_group(step)
    for k in range(4):
        for m in range(4):
            dens[k * BLK : (k + 1) * BLK, m * BLK : (m + 1) * BLK] = (acc[k, m] * factor).astype(
                BF16
            )


def params():
    return pltpu.CompilerParams(vmem_limit_bytes=VMEM_LIMIT)


def cost(flops, size):
    return pl.CostEstimate(flops=flops, bytes_accessed=size, transcendentals=0)


def steps(
    slabs,
    pno_coef,
    dom_blocks,
    pair_first,
    pair_second,
    pno_energy,
    pair_shift,
    margin_i,
    margin_j,
    couple_i,
    couple_j,
    ask_i,
    ask_j,
    link_i,
    link_j,
):
    pairs, domain, pno = pno_coef.shape
    pao, aux = slabs.shape[1:]
    where = jnp.stack([lax.axis_index(a) for a in ALL]).astype(jnp.int32)
    slab = slabs.reshape(pao, aux)
    top = with_asks(slab[: pao // 2], ask_i.reshape(ask_i.shape[1:]))
    bottom = slab[pao // 2 :]
    line = with_asks(slab, ask_j.reshape(ask_j.shape[1:]))
    near_x = neighbours(top, "x")
    near_y = neighbours(bottom, "y")
    lines = [line] + neighbours(line, "z")
    by_x, relay_x, back_x = ring_of_halves(
        jnp.concatenate([top, near_x[0]], axis=0), jnp.concatenate(near_x[1:], axis=0), "y"
    )
    by_y, relay_y, back_y = ring_of_halves(
        jnp.concatenate([bottom, near_y[0]], axis=0), jnp.concatenate(near_y[1:], axis=0), "x"
    )
    lines += across(lines)
    by_x += [shifted(relay_x, "y", 1), shifted(back_x, "y", -1)]
    by_y += [shifted(relay_y, "x", 1), shifted(back_y, "x", -1)]
    pieces = by_x + by_y
    scale = -1.0 / (pno_energy[:, :, None] + pno_energy[:, None, :] + pair_shift[:, None, None])
    coef_t = pno_coef.swapaxes(1, 2)

    block = jax.ShapeDtypeStruct((pairs, pno, pno), F32)
    send_types = [jax.ShapeDtypeStruct((64, pno, pno), BF16)] + [
        jax.ShapeDtypeStruct((4, pno, pno), BF16)
    ] * 8
    fetched = [pltpu.VMEM((pairs, domain, aux), BF16), pltpu.SemaphoreType.DMA((pairs, 2))]
    projected, asked_j = pl.pallas_call(
        first_kernel,
        out_shape=[
            jax.ShapeDtypeStruct((pairs, pno, aux), BF16),
            jax.ShapeDtypeStruct((8, BLK), jnp.int32),
        ],
        in_specs=[SMEM] * 3 + [WHOLE] + [FAR] * 8,
        out_specs=[WHOLE] * 2,
        scratch_shapes=fetched
        + [pltpu.VMEM((8, 16, BLK), BF16), pltpu.SemaphoreType.DMA((8,))],
        compiler_params=params(),
        cost_estimate=cost(pairs * pno * domain * aux * 2, 6 << 20),
        name="project_first",
    )(where, pair_first, dom_blocks, coef_t, *lines)

    exch, asked_i, *sends = pl.pallas_call(
        exchange_kernel,
        out_shape=[block, jax.ShapeDtypeStruct((16, BLK), jnp.int32)] + send_types,
        in_specs=[SMEM] * 4 + [FAR] * 19,
        out_specs=[WHOLE] * 11,
        scratch_shapes=fetched
        + [
            pltpu.VMEM((16, 16, BLK), BF16),
            pltpu.SemaphoreType.DMA((16,)),
            pltpu.VMEM((pairs, pno, pno), BF16),
            pltpu.SMEM((16, BLK), jnp.int32),
            pltpu.SemaphoreType.DMA,
            pltpu.VMEM((pairs, pno, domain), BF16),
            pltpu.VMEM((pairs, pno, aux), BF16),
            pltpu.VMEM((pairs, pno, pno), F32),
            pltpu.SemaphoreType.DMA((3 * GROUPS,)),
        ],
        compiler_params=params(),
        cost_estimate=cost(pairs * pno * domain * aux * 3, 10 << 20),
        name="exchange",
    )(where, pair_second, dom_blocks, asked_j, coef_t, projected, scale, *pieces)

    work = 16 * pairs * pno**3 * 4
    margin = pltpu.VMEM((pairs, 16, pno, pno), BF16)
    values = pltpu.VMEM((pairs, pno, pno), F32)
    first_scratch = [
        margin,
        pltpu.VMEM((64, pno, pno), BF16),
        values,
        values,
        pltpu.SemaphoreType.DMA((1 + 4 * GROUPS,)),
    ]
    for iteration in range(ITERS):
        send_i, send_j = sends[0], sends[1:]
        table_i = lax.all_to_all(
            send_i.reshape(16, 4, pno, pno), IA, split_axis=0, concat_axis=0, tiled=True
        ).reshape(64, pno, pno)
        parts = {0: send_j[0]}
        for d in (6, 2, 7, 3, 4, 5, 1):
            back = ((-(d // 2)) % 4) * 2 + d % 2
            parts[d] = to_peer(send_j[back], back // 2, back % 2)
        base = pl.pallas_call(
            second_kind_kernel,
            out_shape=block,
            in_specs=[SMEM] * 3 + [FAR] * 10,
            out_specs=WHOLE,
            scratch_shapes=[
                margin,
                values,
                pltpu.VMEM((32, pno, pno), BF16),
                pltpu.SemaphoreType.DMA((8 + 2 * GROUPS,)),
            ],
            compiler_params=params(),
            cost_estimate=cost(work, 12 << 20),
            name="couple_second",
        )(where, link_j, couple_j, margin_j, exch, *(parts[d] for d in range(8)))
        large = (margin_i, table_i, base, scale)
        if iteration < ITERS - 1:
            sends = pl.pallas_call(
                middle_kernel,
                out_shape=send_types,
                in_specs=[SMEM] * 5 + [FAR] * 4,
                out_specs=[WHOLE] * 9,
                scratch_shapes=[pltpu.VMEM((pairs, pno, pno), BF16)] + first_scratch,
                compiler_params=params(),
                cost_estimate=cost(work, 14 << 20),
                name="couple_first",
            )(where, link_i, couple_i, asked_i, asked_j, *large)
        else:
            factor = 1.0 / math.sqrt(pairs * lax.axis_size(ALL))
            amplitudes, partial_sum = pl.pallas_call(
                functools.partial(last_kernel, factor),
                out_shape=[block, jax.ShapeDtypeStruct((pao, pao), BF16)],
                in_specs=[SMEM] * 3 + [FAR] * 5,
                out_specs=[WHOLE] * 2,
                scratch_shapes=[pltpu.VMEM((4, 4, BLK, BLK), F32)]
                + first_scratch
                + [pltpu.VMEM((pairs, domain, pno), BF16)],
                compiler_params=params(),
                cost_estimate=cost(work, 16 << 20),
                name="couple_last",
            )(link_i, couple_i, dom_blocks, pno_coef, *large)
    split = partial_sum.reshape(-1, 4, pao)
    got = lax.all_to_all(split, ALL, split_axis=0, concat_axis=0, tiled=True)
    return amplitudes, jnp.sum(got.astype(F32), axis=0)


def solution(mesh):
    split = Mesh(mesh.devices.reshape(4, 4, 4, 2), ALL)
    ranks = (3, 3, 2, 1, 1, 2, 1, 4, 4, 2, 2, 3, 3, 2, 2)
    placed = tuple(P(ALL, *(None,) * (rank - 1)) for rank in ranks)
    return jax.shard_map(
        steps,
        mesh=split,
        in_specs=placed,
        out_specs=(P(ALL, None, None), P(ALL, None)),
        check_vma=False,
    )
```
